512 devices in a mesh: rep: 2 (over y), seq: 32 (over z, core), head: 8 (over x).
Axes of the slice: x: 8, y: 2, z: 16, core: 2. Of those that a mesh axis runs over, the one named last changes fastest.
The devices are a block of a 8x16x16 slice.
Arguments:
- queries: bfloat16 [16384, 4096], P(('rep', 'seq'), 'head'), parts along dimension 0, may hold values from -520 to 520
- rotated_key_states: bfloat16 [16384, 1024], P(('rep', 'seq'), 'head'), parts along dimension 0, may hold values from -6 to 6
- value_state_array: bfloat16 [16384, 1024], P(('rep', 'seq'), 'head'), parts along dimension 0, may hold values from -6 to 6
- residual: bfloat16 [16384, 4096], P(('rep', 'seq'), 'head'), parts along dimension 0, may hold values from -60 to 60
- out_weight: bfloat16 [4096, 4096], P('head'), may hold values from -0.75 to 0.75
- norm_gain: bfloat16 [4096], P('head'), may hold values from 0.5 to 1.5
- block_order: int32 [128], P('rep'), parts along dimension 0, may hold values from 0 to 63, as said below
Outputs:
- normed: bfloat16 [16384, 4096], P(('rep', 'seq'), 'head'), parts along dimension 0
The draws below stay inside these ranges and needn't reach their ends.
There are 2 independent parts, one for each index of `rep`. The reference program is written for one: setup_inputs(seed, part) draws one part's arguments, and reference() takes and returns one part's arrays. A program takes and returns all parts, laid end to end along the dimension named above; an argument that names none is the same for every part. Nothing has to cross between parts.
Inputs may be any that keep to these rules, and one draw needn't show every extreme that they name: `block_order`: slots 2i and 2i + 1 hold blocks c and 63 - c in either order; every block appears once.
All inputs are finite; a program needn't handle non-finite values.
Results may differ from the reference program's by a relative error of at most 0.008.
Values may be sent and summed in bfloat16 or wider, within the bound.
A program may use at most 64 MiB of HBM per device.

```python
import math
import jax
import jax.numpy as jnp
from jax import lax

D = 4096
QUERY_HEADS = 32
KEY_VALUE_HEADS = 8
HEAD_SIZE = 128
SEQUENCE_BLOCK = 128
BLOCKS = 64
SEQUENCE_LENGTH = 8192


def paired_heads(key):
    base_key = jax.random.fold_in(key, 7)
    query_key, random_key_for_keys = jax.random.split(base_key, 2)
    unrotated_queries = jnp.clip(jax.random.normal(query_key, (SEQUENCE_LENGTH, QUERY_HEADS * HEAD_SIZE), jnp.float32) * 1.5, -9.0, 9.0)
    unrotated_keys = jnp.clip(jax.random.normal(random_key_for_keys, (SEQUENCE_LENGTH, KEY_VALUE_HEADS, HEAD_SIZE), jnp.float32), -6.0, 6.0)
    return (unrotated_queries, unrotated_keys.reshape(SEQUENCE_LENGTH, KEY_VALUE_HEADS * HEAD_SIZE))


def draw_queries(key, part):
    return paired_heads(key)[0].astype(jnp.bfloat16)


def draw_rotated_key_states(key, part):
    return paired_heads(key)[1].astype(jnp.bfloat16)


def draw_residual(key, part):
    row_key, column_key, entry_key = jax.random.split(jax.random.fold_in(key, 5), 3)
    row_scale = jnp.exp(jax.random.uniform(row_key, (SEQUENCE_LENGTH, 1), jnp.float32, math.log(0.3), math.log(3.0)))
    column_place = jnp.arange(D, dtype=jnp.float32) / D
    jitter = jax.random.uniform(column_key, (D,), jnp.float32, 0.7, 1.3)
    column_scale = jnp.power(3.0, column_place) * jitter
    entries = jnp.clip(jax.random.normal(entry_key, (SEQUENCE_LENGTH, D), jnp.float32), -5.0, 5.0)
    return (entries * row_scale * column_scale[None, :]).astype(jnp.bfloat16)


def draw_block_order(key, part):
    pair_key, flip_key = jax.random.split(jax.random.fold_in(key, 3))
    pair_count = BLOCKS // 2
    early_ids = jax.random.permutation(pair_key, pair_count).astype(jnp.int32)
    flip_bits = jax.random.randint(flip_key, (pair_count,), 0, 2)
    first_slot = jnp.where(flip_bits == 1, early_ids, BLOCKS - 1 - early_ids)
    second_slot = BLOCKS - 1 - first_slot
    return jnp.stack([first_slot, second_slot], axis=1).reshape(BLOCKS).astype(jnp.int32)


def level_of(own_key, shape, cuts, least, largest):
    factor_of, own = 1.0, jax.random.fold_in(own_key, 6)
    for dim, blocks in cuts:
        heights = jnp.exp(jax.random.uniform(jax.random.fold_in(own, dim), (blocks,), jnp.float32, least / len(cuts), largest / len(cuts)))
        factor_of = factor_of * jnp.repeat(heights, shape[dim] // blocks).reshape([-1 if axis == dim else 1 for axis in range(len(shape))])
    return factor_of


def centred(key, dims, deviation, reach, shards=(), kind=jnp.bfloat16):
    drawn = deviation * jax.random.normal(key, dims, jnp.float32)
    if shards:
        drawn = drawn * level_of(key, dims, shards, -0.22, 0.18)
    return jnp.clip(drawn, -reach, reach).astype(kind)


def setup_inputs(seed: int = 0, part: int = 0) -> dict:
    key_list = jax.random.split(jax.random.key(seed), 8)
    part_splits = jax.random.split(jax.random.fold_in(key_list[7], part), 8)
    return {
        "queries": draw_queries(jax.random.fold_in(jax.random.fold_in(key_list[7], part), 71), part),
        "rotated_key_states": draw_rotated_key_states(jax.random.fold_in(jax.random.fold_in(key_list[7], part), 71), part),
        "value_state_array": centred(part_splits[2], (SEQUENCE_LENGTH, KEY_VALUE_HEADS * HEAD_SIZE), 1.0, 6.0, ((0, 32), (1, 8))),
        "residual": draw_residual(jax.random.fold_in(jax.random.fold_in(key_list[7], part), 71), part),
        "out_weight": centred(key_list[4], (QUERY_HEADS * HEAD_SIZE, D), (HEAD_SIZE // 2) ** -0.5, 0.75, ((0, 8),)),
        "norm_gain": jnp.clip(1.0 + 0.1 * jax.random.normal(key_list[5], (D,), jnp.float32), 0.5, 1.5).astype(jnp.bfloat16),
        "block_order": draw_block_order(jax.random.fold_in(jax.random.fold_in(key_list[7], part), 71), part),
    }


norm_epsilon = 1e-05

def reference(queries, rotated_key_states, value_state_array, residual, out_weight, norm_gain, block_order):
    row_total_count = queries.shape[0]
    row_ids = jnp.arange(row_total_count, dtype=jnp.int32)
    positions = (block_order[row_ids // SEQUENCE_BLOCK] * SEQUENCE_BLOCK + row_ids % SEQUENCE_BLOCK).astype(jnp.int32)
    queries_per_group = QUERY_HEADS // KEY_VALUE_HEADS
    heads_of_keys = rotated_key_states.astype(jnp.float32).reshape(row_total_count, KEY_VALUE_HEADS, HEAD_SIZE)
    heads_of_values = value_state_array.astype(jnp.float32).reshape(row_total_count, KEY_VALUE_HEADS, HEAD_SIZE)
    heads_of_queries = queries.astype(jnp.float32).reshape(row_total_count // SEQUENCE_BLOCK, SEQUENCE_BLOCK, KEY_VALUE_HEADS, queries_per_group, HEAD_SIZE)
    query_positions = positions.reshape(row_total_count // SEQUENCE_BLOCK, SEQUENCE_BLOCK)

    def one_block(packed):
        block_queries, block_positions = packed
        scores = jnp.einsum('qhgd,khd->hgqk', block_queries, heads_of_keys, precision=lax.Precision.HIGHEST) * HEAD_SIZE ** (-0.5)
        visible = (positions[None, :] <= block_positions[:, None])[None, None]
        limited = jnp.where(visible, scores, -1e+30)
        row_peak = lax.optimization_barrier(jnp.max(limited, axis=3, keepdims=True))
        weights = jnp.where(visible, jnp.exp(limited - row_peak), 0.0)
        denominators = lax.optimization_barrier(jnp.sum(weights, axis=3))
        rounded = lax.optimization_barrier(weights.astype(jnp.bfloat16)).astype(jnp.float32)
        weighted_sum = jnp.einsum('hgqk,khd->hgqd', rounded, heads_of_values, precision=lax.Precision.HIGHEST)
        result = weighted_sum / denominators[..., None]
        return result.transpose(2, 0, 1, 3).reshape(SEQUENCE_BLOCK, QUERY_HEADS * HEAD_SIZE).astype(jnp.bfloat16)
    attention = lax.map(one_block, (heads_of_queries, query_positions)).reshape(row_total_count, QUERY_HEADS * HEAD_SIZE)
    mixed_rows = residual.astype(jnp.float32) + jnp.dot(attention, out_weight, preferred_element_type=jnp.float32)
    mean_square = lax.optimization_barrier(jnp.mean(mixed_rows * mixed_rows, axis=1))
    inverse = lax.rsqrt(mean_square + norm_epsilon)
    return (mixed_rows * inverse[:, None] * norm_gain.astype(jnp.float32)[None, :]).astype(jnp.bfloat16)
```

```python
import functools
import math

import jax
import jax.numpy as jnp
from jax import lax
from jax.experimental import pallas as pl
from jax.experimental.pallas import tpu as pltpu
from jax.sharding import PartitionSpec as P

HEAD_SIZE = 128
NORM_EPSILON = 1e-05
BIG = 1e30
MESH = pl.DeviceIdType.MESH
F32 = jnp.float32
BF16 = jnp.bfloat16
SCALE = math.log2(math.e) * HEAD_SIZE ** (-0.5)
RELAY = 1


def kernel(
    dims,
    order_ref, q_ref, k_ref, v_ref, res_ref, w_hbm, gain_ref,
    out_ref,
    wv, qs, kbuf, vbuf, acc, peak, att, xs, xr, mixed, ssq_out, ssq_in,
    wsem, pair_send, pair_recv, ring_send, ring_recv, share_send, xs_sem, xr_sem, n_send, n_recv,
):
    nz, nx, heads, block = dims
    half_z = nz // 2
    rows = heads * block
    width = res_ref.shape[1]
    half = width // 2
    me = lax.axis_index("seq")
    core = lax.rem(me, 2)
    z = me // 2
    hx = lax.axis_index("head")
    sib = z * 2 + 1 - core
    zr = lax.rem(z + 1, nz) * 2 + core
    zl = lax.rem(z + nz - 1, nz) * 2 + core

    w_copy = pltpu.make_async_copy(w_hbm, wv, wsem)
    w_copy.start()

    barrier = pltpu.get_barrier_semaphore()
    for target in (sib, zr, zl):
        pl.semaphore_signal(barrier, inc=1, device_id={"seq": target}, device_id_type=MESH)
    for d in range(1, nx):
        pl.semaphore_signal(
            barrier, inc=1, device_id={"head": lax.rem(hx + d, nx)}, device_id_type=MESH
        )

    swapped = order_ref[2 * me] > order_ref[2 * me + 1]

    def pick(g, ref, cols):
        top, bottom = ref[pl.ds(0, block), cols], ref[pl.ds(block, block), cols]
        return lax.select_n(swapped, *((top, bottom) if g == 0 else (bottom, top)))

    every = slice(None)
    own_half = pl.ds(pl.multiple_of(core * block, block), block)
    sib_half = pl.ds(pl.multiple_of((1 - core) * block, block), block)
    for g in range(2):
        kbuf[g, 0, 0, own_half, :] = pick(g, k_ref, every)
        vbuf[g, 0, 0, own_half, :] = pick(g, v_ref, every)
    bufs = (kbuf, vbuf)

    pl.semaphore_wait(barrier, 2 + nx)

    def pair_copy(g, t):
        return pltpu.make_async_remote_copy(
            src_ref=bufs[t].at[g, 0, 0, own_half, :],
            dst_ref=bufs[t].at[g, 0, 0, own_half, :],
            send_sem=pair_send.at[g, t],
            recv_sem=pair_recv.at[g, t],
            device_id={"seq": sib},
            device_id_type=MESH,
        )

    def ring_copy(g, t, s, d):
        source = bufs[t].at[g, 0, 0] if isinstance(s, int) and s == 0 else bufs[t].at[g, s, d]
        return pltpu.make_async_remote_copy(
            src_ref=source,
            dst_ref=bufs[t].at[g, s + 1, d],
            send_sem=ring_send.at[g, t, s, d],
            recv_sem=ring_recv.at[g, t, s + 1, d],
            device_id={"seq": (zr, zl)[d]},
            device_id_type=MESH,
        )

    def share_copy(g, t, s, d):
        return pltpu.make_async_remote_copy(
            src_ref=bufs[t].at[g, s, d],
            dst_ref=bufs[t].at[g, s, d],
            send_sem=share_send.at[g, t, s, d],
            recv_sem=ring_recv.at[g, t, s, d],
            device_id={"seq": sib},
            device_id_type=MESH,
        )

    def wait_arrival(g, t, s, d):
        pltpu.make_async_copy(
            bufs[t].at[g, s, d], bufs[t].at[g, s, d], ring_recv.at[g, t, s, d]
        ).wait()

    for g in range(2):
        for t in range(2):
            pair_copy(g, t).start()

    for g in range(2):
        for h in range(heads):
            qs[pl.ds(g * rows + h * block, block), :] = pick(
                g, q_ref, pl.ds(h * HEAD_SIZE, HEAD_SIZE)
            )
    peak[...] = jnp.full_like(peak, -BIG)
    acc[...] = jnp.zeros_like(acc)

    for g in range(2):
        for t in range(2):
            pltpu.make_async_copy(
                bufs[t].at[g, 0, 0, sib_half, :],
                bufs[t].at[g, 0, 0, sib_half, :],
                pair_recv.at[g, t],
            ).wait()

            @pl.when(core == RELAY)
            def _(g=g, t=t):
                ring_copy(g, t, 0, 0).start()
                ring_copy(g, t, 0, 1).start()

    def low_of(index):
        a, b = order_ref[2 * index], order_ref[2 * index + 1]
        return jnp.minimum(a, b)

    my_low = low_of(me)

    def hidden(g, index):
        lo = low_of(index)
        seen = (lo < my_low) if g == 0 else (lo > my_low)
        return jnp.where(seen, F32(0.0), F32(BIG))

    tile_rows = min(rows, 256)

    def flash(qg, kc, vc, masks):
        keys = kc.shape[0]
        spans = keys // block
        vext = jnp.concatenate([vc, jnp.ones_like(vc)], axis=1)
        for i in range(rows // tile_rows):
            r = pl.ds(qg * rows + i * tile_rows, tile_rows)
            scores = lax.dot_general(
                qs[r, :], kc, (((1,), (1,)), ((), ())), preferred_element_type=F32
            )
            old = peak[r, :]
            parts = [scores[:, b * block:(b + 1) * block] for b in range(spans)]
            if masks is not None:
                parts = [p if m is None else p - m for p, m in zip(parts, masks)]
            best = functools.reduce(jnp.maximum, parts)
            new = jnp.maximum(old, jnp.max(best, axis=1, keepdims=True))
            weights = jnp.concatenate(
                [jnp.exp2((p - new) * SCALE).astype(BF16) for p in parts], axis=1
            )
            factor = jnp.exp2((old - new) * SCALE)
            peak[r, :] = new
            part = jnp.dot(weights, vext, preferred_element_type=F32)
            acc[r, :] = acc[r, :] * jnp.concatenate([factor, factor], axis=1) + part

    row_id = lax.broadcasted_iota(jnp.int32, (tile_rows, block), 0)
    col_id = lax.broadcasted_iota(jnp.int32, (tile_rows, block), 1)
    triangle = jnp.where(col_id <= lax.rem(row_id, block), F32(0.0), F32(BIG))

    def own_chunk(g, t):
        return jnp.concatenate(
            [bufs[t][g, 0, 0, own_half, :], bufs[t][g, 0, 0, sib_half, :]], axis=0
        )

    low_k, low_v = own_chunk(0, 0), own_chunk(0, 1)
    flash(0, low_k, low_v, [triangle, hidden(0, sib)])
    flash(1, low_k, low_v, None)

    def chunk(g, t, s):
        return jnp.concatenate([bufs[t][g, s, 0], bufs[t][g, s, 1]], axis=0)

    def masks_of(g, s):
        left = lax.rem(z + nz - s, nz)
        right = lax.rem(z + s, nz)
        return [
            hidden(g, 2 * left), hidden(g, 2 * left + 1),
            hidden(g, 2 * right), hidden(g, 2 * right + 1),
        ]

    def receive(g, t, s, last):
        for d in range(2):
            wait_arrival(g, t, s, d)

            @pl.when(core == RELAY)
            def _(d=d):
                if not last or d == t:
                    ring_copy(g, t, s, d).start()
                share_copy(g, t, s, d).start()

    def high_own():
        flash(1, own_chunk(1, 0), own_chunk(1, 1), [triangle, hidden(1, sib)])

    def step(s, last, before):
        receive(0, 0, s, last)
        before()
        receive(0, 1, s, last)
        flash(0, chunk(0, 0, s), chunk(0, 1, s), masks_of(0, s))
        receive(1, 0, s, last)
        flash(1, chunk(0, 0, s), chunk(0, 1, s), None)
        receive(1, 1, s, last)

    def high_step(s):
        flash(1, chunk(1, 0, s), chunk(1, 1, s), masks_of(1, s))

    step(1, half_z == 2, high_own)

    def loop_body(s, carry):
        step(s, False, lambda: high_step(s - 1))
        return carry

    lax.fori_loop(2, half_z - 1, loop_body, 0)
    if half_z > 2:
        step(half_z - 1, True, lambda: high_step(half_z - 2))

    far = lax.rem(z + half_z, nz)

    def receive_last(g, t):
        wait_arrival(g, t, half_z, t)

        @pl.when(core == RELAY)
        def _():
            share_copy(g, t, half_z, t).start()

    def far_masks(g):
        return [hidden(g, 2 * far), hidden(g, 2 * far + 1)]

    def finish(g):
        for h in range(heads):
            r = pl.ds(g * rows + h * block, block)
            att[g, :, pl.ds(h * HEAD_SIZE, HEAD_SIZE)] = (
                acc[r, pl.ds(0, HEAD_SIZE)] / acc[r, pl.ds(HEAD_SIZE, HEAD_SIZE)]
            ).astype(BF16)

    def project(g, owner):
        return jnp.dot(
            att[g],
            wv[:, pl.ds(pl.multiple_of(owner * width, width), width)],
            preferred_element_type=F32,
        )

    def x_copy(g, d, o, p):
        return pltpu.make_async_remote_copy(
            src_ref=xs.at[g, d, o - 1, p],
            dst_ref=xr.at[g, d, o - 1, p],
            send_sem=xs_sem.at[g, d, o - 1, p],
            recv_sem=xr_sem.at[g, d, o - 1, p],
            device_id={"head": lax.rem(hx + (1, nx - 1)[d], nx)},
            device_id_type=MESH,
        )

    half_x = nx // 2
    halves = (pl.ds(0, half), pl.ds(half, half))

    def reduce_stage(g, o):
        if o == half_x:
            own = project(g, lax.rem(hx + o, nx)).astype(BF16)
            for d in range(2):
                xs[g, d, o - 1, d] = own[:, d * half:(d + 1) * half]
                x_copy(g, d, o, d).start()
            return
        for d in range(2):
            own = project(g, lax.rem(hx + (o, nx - o)[d], nx))
            for p in (1 - d, d):
                term = own[:, p * half:(p + 1) * half]
                if o + 1 < half_x or p == d:
                    x_copy(g, d, o + 1, p).wait_recv()
                    term = term + xr[g, d, o, p].astype(F32)
                xs[g, d, o - 1, p] = term.astype(BF16)
                x_copy(g, d, o, p).start()

    def norm_copy(g, d):
        return pltpu.make_async_remote_copy(
            src_ref=ssq_out.at[g],
            dst_ref=ssq_in.at[g, d - 1],
            send_sem=n_send.at[g, d - 1],
            recv_sem=n_recv.at[g, d - 1],
            device_id={"head": lax.rem(hx + d, nx)},
            device_id_type=MESH,
        )

    def reduce_last(g):
        total = project(g, hx) + pick(g, res_ref, every).astype(F32)
        sides = []
        for p in range(2):
            side = total[:, p * half:(p + 1) * half]
            for d in (1 - p, p):
                x_copy(g, d, 1, p).wait_recv()
                side = side + xr[g, d, 0, p].astype(F32)
            mixed[g, :, halves[p]] = side
            sides.append(side)
        squares = sides[0] * sides[0] + sides[1] * sides[1]
        pieces = [squares[:, c * block:(c + 1) * block] for c in range(half // block)]
        column = functools.reduce(jnp.add, pieces)
        row = jnp.sum(column.T, axis=0, keepdims=True)
        ssq_out[g] = jnp.broadcast_to(row, ssq_out.shape[1:])
        for d in range(1, nx):
            norm_copy(g, d).start()

    def output(g):
        total = ssq_out[g]
        for d in range(1, nx):
            norm_copy(g, d).wait_recv()
            total = total + ssq_in[g, d - 1]
        inverse = lax.rsqrt(total / (nx * width) + NORM_EPSILON)
        column = jnp.broadcast_to(inverse[0:1, :], (block, block)).T
        for c in range(width // block):
            cols = pl.ds(c * block, block)
            out_ref[g, :, cols] = (
                mixed[g, :, cols] * column * gain_ref[:, cols].astype(F32)
            ).astype(BF16)

    receive_last(0, 0)
    high_step(half_z - 1)
    receive_last(0, 1)
    low_k, low_v = bufs[0][0, half_z, 0], bufs[1][0, half_z, 1]
    flash(0, low_k, low_v, far_masks(0))
    finish(0)
    w_copy.wait()
    reduce_stage(0, half_x)
    flash(1, low_k, low_v, None)
    receive_last(1, 0)
    receive_last(1, 1)
    flash(1, bufs[0][1, half_z, 0], bufs[1][1, half_z, 1], far_masks(1))
    finish(1)
    reduce_stage(1, half_x)
    for o in range(half_x - 1, 0, -1):
        for g in range(2):
            reduce_stage(g, o)
    reduce_last(0)
    reduce_last(1)
    output(0)
    output(1)

    for g in range(2):
        for t in range(2):
            pair_copy(g, t).wait_send()
        for d in range(1, nx):
            norm_copy(g, d).wait_send()
        for d in range(2):
            for o in range(1, half_x + 1):
                for p in range(2):
                    if o < half_x or p == d:
                        x_copy(g, d, o, p).wait_send()

    @pl.when(core == RELAY)
    def _():
        for g in range(2):
            for t in range(2):
                for d in range(2):
                    ring_copy(g, t, 0, d).wait_send()
                    if d == t:
                        ring_copy(g, t, half_z - 1, d).wait_send()
                        share_copy(g, t, half_z, d).wait_send()
                    share_copy(g, t, half_z - 1, d).wait_send()

        def drain(s, carry):
            for g in range(2):
                for t in range(2):
                    for d in range(2):
                        ring_copy(g, t, s, d).wait_send()
                        share_copy(g, t, s, d).wait_send()
            return carry

        lax.fori_loop(1, half_z - 1, drain, 0)


def body(queries, keys, values, residual, out_weight, norm_gain, block_order):
    nz = lax.axis_size("seq") // 2
    nx = lax.axis_size("head")
    tokens, q_width = queries.shape
    block = tokens // 2
    heads = q_width // HEAD_SIZE
    width = residual.shape[1]
    rows = heads * block
    half_z, half_x = nz // 2, nx // 2
    vmem = pl.BlockSpec(memory_space=pltpu.VMEM)
    dma = pltpu.SemaphoreType.DMA
    result = pl.pallas_call(
        functools.partial(kernel, (nz, nx, heads, block)),
        out_shape=jax.ShapeDtypeStruct((2, block, width), BF16),
        in_specs=[
            pl.BlockSpec(memory_space=pltpu.SMEM), vmem, vmem, vmem, vmem,
            pl.BlockSpec(memory_space=pl.ANY), vmem,
        ],
        out_specs=vmem,
        scratch_shapes=[
            pltpu.VMEM(out_weight.shape, BF16),
            pltpu.VMEM((2 * rows, HEAD_SIZE), BF16),
            pltpu.VMEM((2, half_z + 1, 2, tokens, HEAD_SIZE), BF16),
            pltpu.VMEM((2, half_z + 1, 2, tokens, HEAD_SIZE), BF16),
            pltpu.VMEM((2 * rows, 2 * HEAD_SIZE), F32),
            pltpu.VMEM((2 * rows, block), F32),
            pltpu.VMEM((2, block, q_width), BF16),
            pltpu.VMEM((2, 2, half_x, 2, block, width // 2), BF16),
            pltpu.VMEM((2, 2, half_x, 2, block, width // 2), BF16),
            pltpu.VMEM((2, block, width), F32),
            pltpu.VMEM((2, 8, block), F32),
            pltpu.VMEM((2, nx - 1, 8, block), F32),
            dma,
            dma((2, 2)),
            dma((2, 2)),
            dma((2, 2, half_z, 2)),
            dma((2, 2, half_z + 1, 2)),
            dma((2, 2, half_z + 1, 2)),
            dma((2, 2, half_x, 2)),
            dma((2, 2, half_x, 2)),
            dma((2, nx - 1)),
            dma((2, nx - 1)),
        ],
        compiler_params=pltpu.CompilerParams(
            collective_id=0, has_side_effects=True, vmem_limit_bytes=40 * 1024 * 1024
        ),
    )(
        block_order, queries, keys, values, residual, out_weight,
        norm_gain.reshape(1, width),
    )
    me = lax.axis_index("seq")
    pair = lax.dynamic_slice_in_dim(block_order, 2 * me, 2)
    swapped = pair[0] > pair[1]
    first = jnp.where(swapped, result[1], result[0])
    second = jnp.where(swapped, result[0], result[1])
    return jnp.concatenate([first, second], axis=0)


def solution(mesh):
    split = P(("rep", "seq"), "head")
    return jax.shard_map(
        body,
        mesh=mesh,
        in_specs=(split, split, split, split, P("head", None), P("head"), P("rep")),
        out_specs=split,
        check_vma=False,
    )
```

```python
import functools
import math

import jax
import jax.numpy as jnp
from jax import lax
from jax.experimental import pallas as pl
from jax.experimental.pallas import tpu as pltpu
from jax.sharding import PartitionSpec as P

HEAD_SIZE = 128
NORM_EPSILON = 1e-05
BIG = 1e30
MESH = pl.DeviceIdType.MESH
F32 = jnp.float32
BF16 = jnp.bfloat16
SCALE = math.log2(math.e) * HEAD_SIZE ** (-0.5)


LAG = 4


def kernel(
    dims,
    order_hbm, q_hbm, k_hbm, v_hbm, res_hbm, w_hbm,
    out_ref,
    order_ref, q_in, k_in, v_in, res_ref, wv, qs, kv, acc, peak, att, xs, xr, mixed, ssq_out, ssq_in,
    in_sem, pair_send, pair_recv, ring_send, ring_recv, share_send, xs_sem, xr_sem, n_send, n_recv,
):
    nz, nx, heads, block = dims
    half_z, half_x = nz // 2, nx // 2
    rows = heads * block
    width = res_ref.shape[1]
    half = width // 2
    me = lax.axis_index("seq")
    core = lax.rem(me, 2)
    z = me // 2
    hx = lax.axis_index("head")
    sib = z * 2 + 1 - core
    heading = 2 * core - 1
    mine, other = 1 - core, core
    ahead = lax.rem(z + heading + nz, nz) * 2 + core
    behind = lax.rem(z - heading + nz, nz) * 2 + core
    early = z < half_z

    loads = [
        pltpu.make_async_copy(a, b, in_sem.at[i])
        for i, (a, b) in enumerate(
            [(k_hbm, k_in), (v_hbm, v_in), (order_hbm, order_ref), (q_hbm, q_in),
             (res_hbm, res_ref), (w_hbm, wv)]
        )
    ]
    for load in loads:
        load.start()

    barrier = pltpu.get_barrier_semaphore()
    for target in (behind, sib):
        pl.semaphore_signal(barrier, inc=1, device_id={"seq": target}, device_id_type=MESH)
    for d in range(1, nx):
        pl.semaphore_signal(
            barrier, inc=1, device_id={"head": lax.rem(hx + d, nx)}, device_id_type=MESH
        )

    for load in loads[:3]:
        load.wait()
    swapped = order_ref[2 * me] > order_ref[2 * me + 1]

    def pick(g, ref, cols):
        top, bottom = ref[pl.ds(0, block), cols], ref[pl.ds(block, block), cols]
        return lax.select_n(swapped, *((top, bottom) if g == 0 else (bottom, top)))

    every = slice(None)
    own_half = pl.ds(pl.multiple_of(core * block, block), block)
    sib_half = pl.ds(pl.multiple_of((1 - core) * block, block), block)
    for g in range(2):
        for t, ref in enumerate((k_in, v_in)):
            kv[g, t, 0, 0, own_half, :] = pick(g, ref, every)

    pl.semaphore_wait(barrier, 1 + nx)

    def pair_copy(g, t):
        return pltpu.make_async_remote_copy(
            src_ref=kv.at[g, t, 0, 0, own_half, :],
            dst_ref=kv.at[g, t, 0, 0, own_half, :],
            send_sem=pair_send.at[g, t],
            recv_sem=pair_recv.at[g, t],
            device_id={"seq": sib},
            device_id_type=MESH,
        )

    def ring_copy(g, t, s):
        source = kv.at[g, t, 0, 0] if isinstance(s, int) and s == 0 else kv.at[g, t, s, mine]
        return pltpu.make_async_remote_copy(
            src_ref=source,
            dst_ref=kv.at[g, t, s + 1, mine],
            send_sem=ring_send.at[g, t, s],
            recv_sem=ring_recv.at[g, t, s + 1, mine],
            device_id={"seq": ahead},
            device_id_type=MESH,
        )

    def share_copy(g, t, s):
        return pltpu.make_async_remote_copy(
            src_ref=kv.at[g, t, s, mine],
            dst_ref=kv.at[g, t, s, mine],
            send_sem=share_send.at[g, t, s],
            recv_sem=ring_recv.at[g, t, s, mine],
            device_id={"seq": sib},
            device_id_type=MESH,
        )

    def arrived(g, t, s, d):
        piece = kv.at[g, t, s, d]
        pltpu.make_async_copy(piece, piece, ring_recv.at[g, t, s, d]).wait()

    def pair_arrived(g):
        for t in range(2):
            piece = kv.at[g, t, 0, 0, sib_half, :]
            pltpu.make_async_copy(piece, piece, pair_recv.at[g, t]).wait()

    for g in range(2):
        for t in range(2):
            pair_copy(g, t).start()

    def low_of(index):
        return jnp.minimum(order_ref[2 * index], order_ref[2 * index + 1])

    my_low = low_of(me)

    def hidden(g, plane):
        masks = []
        for c in range(2):
            lo = low_of(2 * plane + c)
            seen = (lo < my_low) if g == 0 else (lo > my_low)
            masks.append(jnp.where(seen, F32(0.0), F32(BIG)))
        return masks

    def hidden_sib(g):
        lo = low_of(sib)
        seen = (lo < my_low) if g == 0 else (lo > my_low)
        return jnp.where(seen, F32(0.0), F32(BIG))

    tile_rows = min(rows, 256)

    def flash(qg, kc, vc, masks):
        keys = kc.shape[0]
        spans = keys // block
        vext = jnp.concatenate([vc, jnp.ones_like(vc)], axis=1)
        for i in range(rows // tile_rows):
            r = pl.ds(qg * rows + i * tile_rows, tile_rows)
            scores = lax.dot_general(
                qs[r, :], kc, (((1,), (1,)), ((), ())), preferred_element_type=F32
            )
            old = peak[r, :]
            parts = [scores[:, b * block:(b + 1) * block] for b in range(spans)]
            if masks is not None:
                parts = [p - m for p, m in zip(parts, masks)]
            best = functools.reduce(jnp.maximum, parts)
            new = jnp.maximum(old, jnp.max(best, axis=1, keepdims=True))
            weights = jnp.concatenate(
                [jnp.exp2((p - new) * SCALE).astype(BF16) for p in parts], axis=1
            )
            factor = jnp.exp2((old - new) * SCALE)
            peak[r, :] = new
            part = jnp.dot(weights, vext, preferred_element_type=F32)
            acc[r, :] = acc[r, :] * jnp.concatenate([factor, factor], axis=1) + part

    def own_chunk(g, t):
        return jnp.concatenate(
            [kv[g, t, 0, 0, own_half, :], kv[g, t, 0, 0, sib_half, :]], axis=0
        )

    def plane_of(s, sign):
        return lax.rem(z + sign * s + nz, nz)

    def low_single(s, d, sign):
        flash(0, kv[0, 0, s, d], kv[0, 1, s, d], hidden(0, plane_of(s, sign)))

    def both(g, t, s):
        return jnp.concatenate([kv[g, t, s, 0], kv[g, t, s, 1]], axis=0)

    def relay(g, s, last):
        for t in range(2):
            arrived(g, t, s, mine)
            if not last:
                ring_copy(g, t, s).start()
            share_copy(g, t, s).start()
        if last:
            ring_copy(g, mine, s).start()

    def relay_far(g):
        arrived(g, mine, half_z, mine)
        share_copy(g, mine, half_z).start()

    loads[3].wait()
    for g in range(2):
        for h in range(heads):
            qs[pl.ds(g * rows + h * block, block), :] = pick(
                g, q_in, pl.ds(h * HEAD_SIZE, HEAD_SIZE)
            )
    peak[...] = jnp.full_like(peak, -BIG)
    acc[...] = jnp.zeros_like(acc)

    pair_arrived(0)
    for t in range(2):
        ring_copy(0, t, 0).start()
    pair_arrived(1)

    @pl.when(core == 0)
    def _():
        for t in range(2):
            ring_copy(1, t, 0).start()

    row_id = lax.broadcasted_iota(jnp.int32, (tile_rows, block), 0)
    col_id = lax.broadcasted_iota(jnp.int32, (tile_rows, block), 1)
    triangle = jnp.where(col_id <= lax.rem(row_id, block), F32(0.0), F32(BIG))

    low_k, low_v = own_chunk(0, 0), own_chunk(0, 1)
    flash(0, low_k, low_v, [triangle, hidden_sib(0)])
    flash(1, low_k, low_v, None)
    flash(1, own_chunk(1, 0), own_chunk(1, 1), [triangle, hidden_sib(1)])

    def other_low(s):
        for t in range(2):
            arrived(0, t, s, other)
        low_single(s, other, heading)

    last_step = half_z - 1
    lag = min(LAG, last_step - 1)

    def low_step(s, last, lagged):
        relay(0, s, last)
        low_single(s, mine, -heading)
        if lagged:
            other_low(s - lag)

        @pl.when(core == 0)
        def _():
            relay(1, s, last)

    def loop(first, stop, step):
        def body_of(s, carry):
            step(s)
            return carry

        lax.fori_loop(first, stop, body_of, 0)

    loop(1, lag + 1, lambda s: low_step(s, False, False))
    loop(lag + 1, last_step, lambda s: low_step(s, False, True))
    low_step(last_step, True, True)
    relay_far(0)

    @pl.when(core == 0)
    def _():
        relay_far(1)

    def high_relays():
        loop(1, last_step, lambda s: relay(1, s, False))
        relay(1, last_step, True)
        relay_far(1)

    @pl.when(core == 1)
    def _():
        for t in range(2):
            ring_copy(1, t, 0).start()

    @pl.when(jnp.logical_and(core == 1, jnp.logical_not(early)))
    def _():
        high_relays()

    loop(last_step - lag + 1, half_z, other_low)
    arrived(0, other, half_z, other)
    far_k, far_v = kv[0, 0, half_z, 0], kv[0, 1, half_z, 1]
    far_plane = plane_of(half_z, 1)
    flash(0, far_k, far_v, hidden(0, far_plane))

    def finish(g):
        for h in range(heads):
            r = pl.ds(g * rows + h * block, block)
            att[g, :, pl.ds(h * HEAD_SIZE, HEAD_SIZE)] = (
                acc[r, pl.ds(0, HEAD_SIZE)] / acc[r, pl.ds(HEAD_SIZE, HEAD_SIZE)]
            ).astype(BF16)

    def project(g, owner):
        return jnp.dot(
            att[g],
            wv[:, pl.ds(pl.multiple_of(owner * width, width), width)],
            preferred_element_type=F32,
        )

    def x_copy(g, d, o, p):
        return pltpu.make_async_remote_copy(
            src_ref=xs.at[g, d, o - 1, p],
            dst_ref=xr.at[g, d, o - 1, p],
            send_sem=xs_sem.at[g, d, o - 1, p],
            recv_sem=xr_sem.at[g, d, o - 1, p],
            device_id={"head": lax.rem(hx + (1, nx - 1)[d], nx)},
            device_id_type=MESH,
        )

    halves = (pl.ds(0, half), pl.ds(half, half))

    def reduce_stage(g, o):
        if o == half_x:
            own = project(g, lax.rem(hx + o, nx)).astype(BF16)
            for d in range(2):
                xs[g, d, o - 1, d] = own[:, d * half:(d + 1) * half]
                x_copy(g, d, o, d).start()
            return
        for d in range(2):
            own = project(g, lax.rem(hx + (o, nx - o)[d], nx))
            for p in (1 - d, d):
                term = own[:, p * half:(p + 1) * half]
                if o + 1 < half_x or p == d:
                    x_copy(g, d, o + 1, p).wait_recv()
                    term = term + xr[g, d, o, p].astype(F32)
                xs[g, d, o - 1, p] = term.astype(BF16)
                x_copy(g, d, o, p).start()

    def norm_copy(g, d):
        return pltpu.make_async_remote_copy(
            src_ref=ssq_out.at[g],
            dst_ref=ssq_in.at[g, d - 1],
            send_sem=n_send.at[g, d - 1],
            recv_sem=n_recv.at[g, d - 1],
            device_id={"head": lax.rem(hx + d, nx)},
            device_id_type=MESH,
        )

    def reduce_last(g):
        total = project(g, hx) + pick(g, res_ref, every).astype(F32)
        sides = []
        for p in range(2):
            side = total[:, p * half:(p + 1) * half]
            for d in (1 - p, p):
                x_copy(g, d, 1, p).wait_recv()
                side = side + xr[g, d, 0, p].astype(F32)
            mixed[g, :, halves[p]] = side
            sides.append(side)
        squares = sides[0] * sides[0] + sides[1] * sides[1]
        pieces = [squares[:, c * block:(c + 1) * block] for c in range(half // block)]
        column = functools.reduce(jnp.add, pieces)
        row = jnp.sum(column.T, axis=0, keepdims=True)
        ssq_out[g] = jnp.broadcast_to(row, ssq_out.shape[1:])
        for d in range(1, nx):
            norm_copy(g, d).start()

    def normalize(g):
        total = ssq_out[g]
        for d in range(1, nx):
            norm_copy(g, d).wait_recv()
            total = total + ssq_in[g, d - 1]
        inverse = lax.rsqrt(total / (nx * width) + NORM_EPSILON)
        column = jnp.broadcast_to(inverse[0:1, :], (block, block)).T
        for c in range(width // block):
            cols = pl.ds(c * block, block)
            mixed[g, :, cols] = mixed[g, :, cols] * column

    finish(0)
    loads[5].wait()
    loads[4].wait()
    reduce_stage(0, half_x)
    flash(1, far_k, far_v, None)

    def high_step(s, last):
        @pl.when(jnp.logical_and(core == 1, early))
        def _():
            relay(1, s, last)

        flash(1, both(0, 0, s), both(0, 1, s), None)
        for t in range(2):
            arrived(1, t, s, other)
        flash(
            1, both(1, 0, s), both(1, 1, s),
            hidden(1, plane_of(s, -1)) + hidden(1, plane_of(s, 1)),
        )

    cuts = [1 + (last_step - 1) * i // half_x for i in range(half_x + 1)]
    for i in range(half_x):
        loop(cuts[i], cuts[i + 1], lambda s: high_step(s, False))
        if half_x - 1 - i > 0:
            reduce_stage(0, half_x - 1 - i)
    high_step(last_step, True)

    @pl.when(jnp.logical_and(core == 1, early))
    def _():
        relay_far(1)

    arrived(1, other, half_z, other)
    flash(1, kv[1, 0, half_z, 0], kv[1, 1, half_z, 1], hidden(1, far_plane))
    finish(1)
    reduce_stage(1, half_x)
    reduce_last(0)
    for o in range(half_x - 1, 0, -1):
        reduce_stage(1, o)
    normalize(0)
    reduce_last(1)
    normalize(1)
    for g in range(2):
        for c in range(width // block):
            cols = pl.ds(c * block, block)
            low, high = mixed[0, :, cols], mixed[1, :, cols]
            out_ref[pl.ds(g * block, block), cols] = lax.select_n(
                swapped, *((low, high) if g == 0 else (high, low))
            )

    for g in range(2):
        for t in range(2):
            pair_copy(g, t).wait_send()
            ring_copy(g, t, 0).wait_send()
            share_copy(g, t, last_step).wait_send()
        ring_copy(g, mine, last_step).wait_send()
        share_copy(g, mine, half_z).wait_send()
        for d in range(1, nx):
            norm_copy(g, d).wait_send()
        for d in range(2):
            for o in range(1, half_x + 1):
                for p in range(2):
                    if o < half_x or p == d:
                        x_copy(g, d, o, p).wait_send()

    def drain(s):
        for g in range(2):
            for t in range(2):
                ring_copy(g, t, s).wait_send()
                share_copy(g, t, s).wait_send()

    loop(1, last_step, drain)


def body(queries, keys, values, residual, out_weight, norm_gain, block_order):
    nz = lax.axis_size("seq") // 2
    nx = lax.axis_size("head")
    tokens, q_width = queries.shape
    block = tokens // 2
    heads = q_width // HEAD_SIZE
    width = residual.shape[1]
    rows = heads * block
    half_z, half_x = nz // 2, nx // 2
    vmem = pl.BlockSpec(memory_space=pltpu.VMEM)
    hbm = pl.BlockSpec(memory_space=pltpu.HBM)
    dma = pltpu.SemaphoreType.DMA
    result = pl.pallas_call(
        functools.partial(kernel, (nz, nx, heads, block)),
        out_shape=jax.ShapeDtypeStruct((tokens, width), F32),
        in_specs=[hbm] * 6,
        out_specs=vmem,
        scratch_shapes=[
            pltpu.SMEM(block_order.shape, jnp.int32),
            pltpu.VMEM(queries.shape, BF16),
            pltpu.VMEM(keys.shape, BF16),
            pltpu.VMEM(values.shape, BF16),
            pltpu.VMEM(residual.shape, BF16),
            pltpu.VMEM(out_weight.shape, BF16),
            pltpu.VMEM((2 * rows, HEAD_SIZE), BF16),
            pltpu.VMEM((2, 2, half_z + 1, 2, tokens, HEAD_SIZE), BF16),
            pltpu.VMEM((2 * rows, 2 * HEAD_SIZE), F32),
            pltpu.VMEM((2 * rows, block), F32),
            pltpu.VMEM((2, block, q_width), BF16),
            pltpu.VMEM((2, 2, half_x, 2, block, width // 2), BF16),
            pltpu.VMEM((2, 2, half_x, 2, block, width // 2), BF16),
            pltpu.VMEM((2, block, width), F32),
            pltpu.VMEM((2, 8, block), F32),
            pltpu.VMEM((2, nx - 1, 8, block), F32),
            dma((6,)),
            dma((2, 2)),
            dma((2, 2)),
            dma((2, 2, half_z)),
            dma((2, 2, half_z + 1, 2)),
            dma((2, 2, half_z + 1)),
            dma((2, 2, half_x, 2)),
            dma((2, 2, half_x, 2)),
            dma((2, nx - 1)),
            dma((2, nx - 1)),
        ],
        compiler_params=pltpu.CompilerParams(
            collective_id=0, has_side_effects=True, vmem_limit_bytes=40 * 1024 * 1024
        ),
    )(block_order, queries, keys, values, residual, out_weight)
    return (result * norm_gain.astype(F32)[None, :]).astype(BF16)


def solution(mesh):
    split = P(("rep", "seq"), "head")
    return jax.shard_map(
        body,
        mesh=mesh,
        in_specs=(split, split, split, split, P("head", None), P("head"), P("rep")),
        out_specs=split,
        check_vma=False,
    )
```
